32 devices in a mesh: tm: 4 (over x, core), space: 8 (over z, y).
Axes of the slice: x: 2, y: 2, z: 4, core: 2. Of those that a mesh axis runs over, the one named last changes fastest.
Arguments:
- start_value: float32 [4, 8, 512, 256], P('tm', 'space'), may hold values from -6 to 6
- old_nodes: float32 [4, 3, 8, 512, 256], P('tm', None, 'space'), may hold values from -6 to 6
- diffusivity: float32 [8, 512, 256], P('space'), may hold values from 0.2 to 2
Outputs:
- fine_nodes: float32 [4, 3, 8, 512, 256], P('tm', None, 'space')
- next_start: float32 [4, 8, 512, 256], P('tm', 'space')
- next_coarse: float32 [4, 8, 512, 256], P('tm', 'space')
The draws below stay inside these ranges and needn't reach their ends.
All inputs are finite; a program needn't handle non-finite values.
Results may differ from the reference program's by a relative error of at most 0.0001.
Values sent between devices are 32-bit elements; how exact they have to be, the bound alone decides.
No kernel may reach another device: no remote copies, remote signals or barrier semaphores. Data moves between devices by JAX's collectives and lax.ppermute only.
A program may use at most 64 MiB of HBM per device.

```python
import math
import jax
import jax.numpy as jnp
from jax import lax

NY = 512
NZ = 256
NODES = 3
CG_ITERS = 2
NX = 8
SLICES = 4


def shard_levels(key, extent, split, low, largest):
    factor_of = 1.0
    for dim, parts in split:
        heights = jax.random.uniform(jax.random.fold_in(jax.random.fold_in(key, 6), dim), (parts,), jnp.float32, low / len(split), largest / len(split))
        factor_of = factor_of * jnp.repeat(jnp.exp(heights), extent[dim] // parts).reshape((-1,) + (1,) * (len(extent) - 1 - dim))
    return factor_of


def bell_draw(own_key, shape, scale, most, cuts=(), kind=jnp.bfloat16):
    array = scale * jax.random.normal(own_key, shape, jnp.float32)
    if cuts:
        array = array * shard_levels(own_key, shape, cuts, -0.22, 0.18)
    return jnp.clip(array, -most, most).astype(kind)


def setup_inputs(seed: int = 0) -> dict:
    streams_of = jax.random.split(jax.random.key(seed), 4)
    start_value = bell_draw(streams_of[0], (SLICES, NX, NY, NZ), 1.0, 6.0, ((0, 4), (1, 8)), jnp.float32)
    old_nodes = bell_draw(streams_of[1], (SLICES, NODES, NX, NY, NZ), 1.0, 6.0, ((0, 4), (2, 8)), jnp.float32)
    diffusivity = jnp.clip(jnp.exp(math.log(2.0) - 2.3025851 * jax.random.uniform(streams_of[2], (NX, NY, NZ), jnp.float32) ** shard_levels(streams_of[2], (NX, NY, NZ), ((0, 8),), -0.2, 0.2)), 0.2, 2.0)
    return dict(start_value=start_value, old_nodes=old_nodes, diffusivity=diffusivity)


STEP = 2.0
ROOT_SIX = math.sqrt(6.0)
NODE_TIMES = [(4.0 - ROOT_SIX) / 10.0, (4.0 + ROOT_SIX) / 10.0, 1.0]
COLLOC = [[(88.0 - 7.0 * ROOT_SIX) / 360.0, (296.0 - 169.0 * ROOT_SIX) / 1800.0, (-2.0 + 3.0 * ROOT_SIX) / 225.0], [(296.0 + 169.0 * ROOT_SIX) / 1800.0, (88.0 + 7.0 * ROOT_SIX) / 360.0, (-2.0 - 3.0 * ROOT_SIX) / 225.0], [(16.0 - ROOT_SIX) / 36.0, (16.0 + ROOT_SIX) / 36.0, 1.0 / 9.0]]

def sweep_weight(row, column):
    below = COLLOC[row - 1][column] if row > 0 else 0.0
    return COLLOC[row][column] - below

def node_width(row):
    below = NODE_TIMES[row - 1] if row > 0 else 0.0
    return NODE_TIMES[row] - below

def neighbour(field, dim, forward):
    length = field.shape[dim]
    edge = jnp.zeros_like(lax.slice_in_dim(field, 0, 1, axis=dim))
    if forward:
        return jnp.concatenate([lax.slice_in_dim(field, 1, length, axis=dim), edge], axis=dim)
    return jnp.concatenate([edge, lax.slice_in_dim(field, 0, length - 1, axis=dim)], axis=dim)

def face_table(kappa):
    faces = []
    for dim in range(3):
        for forward in (True, False):
            faces.append(0.5 * (kappa + neighbour(kappa, dim, forward)))
    total = faces[0] + faces[1] + faces[2] + faces[3] + faces[4] + faces[5]
    return (faces, total)

def apply_heat(field, faces, total):
    result = faces[0] * neighbour(field, 0, True) + faces[1] * neighbour(field, 0, False)
    result = result + faces[2] * neighbour(field, 1, True) + faces[3] * neighbour(field, 1, False)
    result = result + faces[4] * neighbour(field, 2, True) + faces[5] * neighbour(field, 2, False)
    return result - total * field

def combine(weights, images):
    summed = weights[0] * images[0]
    for column in range(1, 3):
        summed = summed + weights[column] * images[column]
    return summed

def solve(guess, residual, width, faces, total):
    iterate = guess
    direction = residual
    norm_now = jnp.sum(residual * residual)
    for sweep in range(CG_ITERS):
        product = direction - width * apply_heat(direction, faces, total)
        step_size = norm_now / jnp.sum(direction * product)
        iterate = iterate + step_size * direction
        if sweep + 1 < CG_ITERS:
            residual = residual - step_size * product
            norm_next = jnp.sum(residual * residual)
            direction = residual + norm_next / norm_now * direction
            norm_now = norm_next
    return iterate

def reference(start_value, old_nodes, diffusivity):
    faces, total = face_table(diffusivity)

    def one_slice(pair):
        begin, previous_nodes = pair
        images = [apply_heat(previous_nodes[column], faces, total) for column in range(3)]
        previous = begin
        fresh = []
        for row in range(3):
            weights = [sweep_weight(row, column) for column in range(3)]
            residual = previous - previous_nodes[row] + STEP * combine(weights, images)
            result = solve(previous_nodes[row], residual, STEP * node_width(row), faces, total)
            fresh.append(result)
            previous = result
        coarse_res = begin - previous_nodes[2] + STEP * combine(COLLOC[2], images)
        coarse_end = solve(previous_nodes[2], coarse_res, STEP, faces, total)
        return (jnp.stack(fresh), coarse_end)
    fine_nodes, coarse_ends = lax.map(one_slice, (start_value, old_nodes))
    next_start = jnp.concatenate([start_value[:1], fine_nodes[:-1, 2]], axis=0)
    next_coarse = jnp.concatenate([start_value[:1], coarse_ends[:-1]], axis=0)
    return (fine_nodes, next_start, next_coarse)
```

```python
import math

import jax
import jax.numpy as jnp
from jax import lax
from jax.experimental import pallas as pl
from jax.experimental.pallas import tpu as pltpu
from jax.sharding import PartitionSpec as P

AXES = ("tm", "space")
STEP = 2.0
ROOT_SIX = math.sqrt(6.0)
NODE_TIMES = [(4.0 - ROOT_SIX) / 10.0, (4.0 + ROOT_SIX) / 10.0, 1.0]
COLLOC = [
    [
        (88.0 - 7.0 * ROOT_SIX) / 360.0,
        (296.0 - 169.0 * ROOT_SIX) / 1800.0,
        (-2.0 + 3.0 * ROOT_SIX) / 225.0,
    ],
    [
        (296.0 + 169.0 * ROOT_SIX) / 1800.0,
        (88.0 + 7.0 * ROOT_SIX) / 360.0,
        (-2.0 - 3.0 * ROOT_SIX) / 225.0,
    ],
    [(16.0 - ROOT_SIX) / 36.0, (16.0 + ROOT_SIX) / 36.0, 1.0 / 9.0],
]
ROWS = 16
KINDS = 16
LANES = 128


def sweep_weight(row, column):
    below = COLLOC[row - 1][column] if row > 0 else 0.0
    return COLLOC[row][column] - below


def node_width(row):
    below = NODE_TIMES[row - 1] if row > 0 else 0.0
    return NODE_TIMES[row] - below


class Places:
    def __init__(self, slices, planes):
        self.slices, self.planes = slices, planes
        self.crossed = slices % 2 == 0 and planes % 2 == 0

    def flat(self, t, s):
        return t * self.planes + s

    def device(self, t, p):
        if not self.crossed:
            return self.flat(t, p)
        return self.flat(2 * (t // 2) + p % 2, 2 * (p // 2) + t % 2)

    def every(self):
        return [(t, p) for t in range(self.slices) for p in range(self.planes)]

    def swap(self):
        return [(self.flat(t, p), self.device(t, p)) for t, p in self.every()]

    def to_next(self):
        return [(self.device(t, p), self.flat(t + 1, p)) for t, p in self.every() if t + 1 < self.slices]

    def pairs(self, odd):
        partner = lambda p: p + 1 if p % 2 == odd else p - 1
        return [
            (self.device(t, p), self.device(t, partner(p)))
            for t, p in self.every()
            if 0 <= partner(p) < self.planes
        ]

    def rounds(self):
        left, stride, found = self.planes, 1, []
        while left > 1:
            factor = next(f for f in range(2, left + 1) if left % f == 0)
            turns = []
            for turn in range(1, factor):
                moved = lambda p: p + (((p // stride + turn) % factor) - (p // stride) % factor) * stride
                turns.append([(self.device(t, p), self.device(t, moved(p))) for t, p in self.every()])
            found.append(turns)
            left, stride = left // factor, stride * factor
        return found


def own_plane(places):
    t, s = lax.axis_index("tm"), lax.axis_index("space")
    return 2 * (s // 2) + t % 2 if places.crossed else s


def move(value, perm):
    return lax.ppermute(value, AXES, perm)


def row_after(ref, lead, start, count):
    total = ref.shape[-2]
    if start + count + 1 <= total:
        return ref[(*lead, slice(start + 1, start + count + 1), slice(None))]
    return pltpu.roll(ref[(*lead, slice(start, start + count), slice(None))], count - 1, 0)


def row_before(ref, lead, start, count):
    if start > 0:
        return ref[(*lead, slice(start - 1, start + count - 1), slice(None))]
    return pltpu.roll(ref[(*lead, slice(0, count), slice(None))], 1, 0)


def heat_rows(own, lead, beside, faces, start, count):
    rows = slice(start, start + count)
    here = own[(*lead, rows, slice(None))]
    width = here.shape[-1]
    face_x = faces[3, rows, :]
    result = faces[0, rows, :] * beside[0] + faces[1, rows, :] * beside[1]
    result += faces[2, rows, :] * row_after(own, lead, start, count)
    lower = row_before(faces, (2,), start, count) * row_before(own, lead, start, count)
    if start == 0:
        lower = jnp.where(lax.broadcasted_iota(jnp.int32, lower.shape, 0) == 0, 0.0, lower)
    result += lower
    result += face_x * pltpu.roll(here, width - 1, 1) + pltpu.roll(face_x * here, 1, 1)
    return result - faces[4, rows, :] * here, here


def chunks(ref):
    total = ref.shape[-2]
    return [(start, min(ROWS, total - start)) for start in range(0, total, ROWS)]


def faces_kernel(kappa, kappa_a, kappa_b, faces):
    length, width = kappa.shape
    for start, count in chunks(kappa):
        rows = slice(start, start + count)
        here = kappa[rows, :]
        face_a = 0.5 * (here + kappa_a[rows, :])
        face_b = 0.5 * (here + kappa_b[rows, :])
        after = row_after(kappa, (), start, count)
        before = row_before(kappa, (), start, count)
        row = lax.broadcasted_iota(jnp.int32, here.shape, 0) + start
        column = lax.broadcasted_iota(jnp.int32, here.shape, 1)
        after = jnp.where(row == length - 1, 0.0, after)
        before = jnp.where(row == 0, 0.0, before)
        right = jnp.where(column == width - 1, 0.0, pltpu.roll(here, width - 1, 1))
        left = jnp.where(column == 0, 0.0, pltpu.roll(here, 1, 1))
        face_y = 0.5 * (here + after)
        face_x = 0.5 * (here + right)
        faces[0, rows, :] = face_a
        faces[1, rows, :] = face_b
        faces[2, rows, :] = jnp.where(row == length - 1, 0.0, face_y)
        faces[3, rows, :] = jnp.where(column == width - 1, 0.0, face_x)
        faces[4, rows, :] = face_a + face_b + face_y + face_x + 0.5 * (here + before) + 0.5 * (here + left)


def increments_kernel(begin, *refs):
    nodes, beside_a, beside_b, faces, outs = refs[:3], refs[3:6], refs[6:9], refs[9], refs[10:]
    for start, count in chunks(begin):
        rows = slice(start, start + count)
        images, values = [], [begin[rows, :]]
        for column in range(3):
            image, here = heat_rows(
                nodes[column], (), (beside_a[column][rows, :], beside_b[column][rows, :]), faces, start, count
            )
            images.append(image)
            values.append(here)
        for row in range(3):
            change = values[row] - values[row + 1]
            for column in range(3):
                change += (STEP * sweep_weight(row, column)) * images[column]
            outs[row][rows, :] = change


def apply_kernel(width, count_in, *refs):
    own, beside_a, beside_b = refs[:count_in], refs[count_in : 2 * count_in], refs[2 * count_in : 3 * count_in]
    faces, out = refs[3 * count_in], refs[3 * count_in + 1 :]
    field = own[0]
    if count_in > 1:
        field = out[1]
        for start, count in chunks(field):
            rows = slice(start, start + count)
            field[rows, :] = sum(ref[rows, :] for ref in own)
    for start, count in chunks(field):
        rows = slice(start, start + count)
        beside = (sum(ref[rows, :] for ref in beside_a), sum(ref[rows, :] for ref in beside_b))
        image, here = heat_rows(field, (), beside, faces, start, count)
        out[0][rows, :] = here - width * image


def folded(value):
    return jnp.sum(value.reshape(value.shape[0] // 8, 8, value.shape[1]), axis=0)


def whole_sum(value):
    return jnp.sum(jnp.sum(value, axis=0, keepdims=True), axis=1, keepdims=True)


def moments_kernel(width, place, residual, image, image_a, image_b, faces, out):
    zero = jnp.zeros((8, residual.shape[1]), jnp.float32)
    rr, rq, qq = zero, zero, zero
    for start, count in chunks(residual):
        rows = slice(start, start + count)
        r, q = residual[rows, :], image[rows, :]
        rr, rq, qq = rr + folded(r * r), rq + folded(r * q), qq + folded(q * q)
    rr, rq, qq = whole_sum(rr), whole_sum(rq), whole_sum(qq)
    centre = jnp.where(qq > 0.0, rq / jnp.where(qq > 0.0, qq, 1.0), 0.0)
    sums = [zero] * 6
    for start, count in chunks(residual):
        rows = slice(start, start + count)
        heat, q = heat_rows(image, (), (image_a[rows, :], image_b[rows, :]), faces, start, count)
        aq = q - width * heat
        w = residual[rows, :] - centre * q
        aw = q - centre * aq
        terms = (w * w, w * q, w * aw, w * aq, q * aw, q * aq)
        sums = [total + folded(term) for total, term in zip(sums, terms)]
    values = [rr, rq, qq, centre] + [whole_sum(total) for total in sums]
    kind = lax.broadcasted_iota(jnp.int32, out.shape, 0)
    lane = lax.broadcasted_iota(jnp.int32, out.shape, 1)
    message = jnp.zeros(out.shape, jnp.float32)
    for index, value in enumerate(values):
        message = jnp.where(kind == index, value, message)
    out[...] = jnp.where(lane == place[0], message, 0.0)


def step_weights(gathered):
    row = lambda index: gathered[index : index + 1, :]
    total = lambda value: jnp.sum(value, axis=1, keepdims=True)
    rr, rq = total(row(0)), total(row(1))
    step = rr / rq
    away = step - row(3)
    rr_next = total(row(4) - 2.0 * away * row(5) + away * away * row(2))
    energy = total(row(6) - away * (row(7) + row(8)) + away * away * row(9))
    momentum = rr_next / rr
    step_next = rr_next / (energy - momentum * rr_next / step)
    return step + step_next * (1.0 + momentum), -step_next * step


def advance_kernel(width, keep, gathered, guess, *refs):
    grown, residual, image, faces = refs[0:3], refs[3:6], refs[6:9], refs[9]
    result, product, following = refs[10], refs[11], refs[12:]
    first, second = step_weights(gathered[...])
    for start, count in chunks(guess):
        rows = slice(start, start + count)
        change = first * residual[0][rows, :] + second * image[0][rows, :]
        result[rows, :] = guess[rows, :] + change
        following[0][rows, :] = grown[0][rows, :] + change
    for start, count in chunks(guess):
        rows = slice(start, start + count)
        beside = []
        for side in (1, 2):
            value = grown[side][rows, :] + first * residual[side][rows, :] + second * image[side][rows, :]
            if keep:
                following[side][rows, :] = value
            beside.append(value)
        heat, here = heat_rows(following[0], (), beside, faces, start, count)
        product[rows, :] = here - width * heat


def finish_kernel(gathered, guess, residual, image, out):
    first, second = step_weights(gathered[...])
    for start, count in chunks(guess):
        rows = slice(start, start + count)
        out[rows, :] = guess[rows, :] + first * residual[rows, :] + second * image[rows, :]


VMEM = pl.BlockSpec(memory_space=pltpu.VMEM)
SMEM = pl.BlockSpec(memory_space=pltpu.SMEM)


def call(kernel, shapes, *args, scalars=0):
    single = not isinstance(shapes, list)
    outs = [jax.ShapeDtypeStruct(shape, jnp.float32) for shape in ([shapes] if single else shapes)]
    found = pl.pallas_call(
        kernel,
        out_shape=outs,
        in_specs=[SMEM] * scalars + [VMEM] * (len(args) - scalars),
        out_specs=[VMEM] * len(outs),
    )(*args)
    return found[0] if single else found


def on_device(places, start_value, old_nodes, diffusivity):
    plane = diffusivity.shape[1:]
    swap, near, far = places.swap(), places.pairs(0), places.pairs(1)
    place = own_plane(places).astype(jnp.int32).reshape(1)

    def sides(value):
        return move(value, far), move(value, near)

    def gather(message):
        for turns in places.rounds():
            message = sum([move(message, perm) for perm in turns], message)
        return message

    def moments(width, residual, image, beside, faces):
        lanes = LANES * (-(-places.planes // LANES))
        return call(
            lambda *refs: moments_kernel(width, *refs),
            (KINDS, lanes),
            place,
            residual,
            image,
            *beside,
            faces,
            scalars=1,
        )

    kappa = move(diffusivity[0], swap)
    nodes = [move(old_nodes[0, column, 0], swap) for column in range(3)]
    begin = move(start_value[0, 0], swap)
    kappa_sides = sides(kappa)
    node_sides = [sides(node) for node in nodes]
    faces = call(faces_kernel, (5, *plane), kappa, *kappa_sides)
    grown = call(
        increments_kernel,
        [plane] * 3,
        begin,
        *nodes,
        *[pair[0] for pair in node_sides],
        *[pair[1] for pair in node_sides],
        faces,
    )
    grown_sides = [sides(value) for value in grown]
    trio = [(grown[m], *grown_sides[m]) for m in range(3)]
    widths = [STEP * node_width(row) for row in range(3)]

    residual = trio[0]
    image = call(lambda *refs: apply_kernel(widths[0], 1, *refs), plane, *residual, faces)
    image_trio = (image, *sides(image))
    fresh = []
    for row in range(2):
        gathered = gather(moments(widths[row], residual[0], image, image_trio[1:], faces))
        keep = row == 0
        found = call(
            lambda *refs: advance_kernel(widths[row + 1], keep, *refs),
            [plane] * (5 if keep else 3),
            gathered,
            nodes[row],
            *trio[row + 1],
            *residual,
            *image_trio,
            faces,
        )
        fresh.append(found[0])
        image, residual = found[1], found[2:]
        image_trio = (image, *sides(image))
    gathered = gather(moments(widths[2], residual[0], image, image_trio[1:], faces))
    fresh.append(call(finish_kernel, plane, gathered, nodes[2], residual[0], image))

    coarse_image, coarse = call(
        lambda *refs: apply_kernel(STEP, 3, *refs),
        [plane] * 2,
        *grown,
        *[pair[0] for pair in grown_sides],
        *[pair[1] for pair in grown_sides],
        faces,
    )
    coarse_gathered = gather(moments(STEP, coarse, coarse_image, sides(coarse_image), faces))
    coarse_end = call(finish_kernel, plane, coarse_gathered, nodes[2], coarse, coarse_image)

    next_coarse = move(coarse_end, places.to_next())
    next_start = move(fresh[2], places.to_next())
    fine_nodes = jnp.stack([move(value, swap) for value in fresh])[None, :, None]
    first_slice = lax.axis_index("tm") == 0
    next_start = jnp.where(first_slice, start_value, next_start[None, None])
    next_coarse = jnp.where(first_slice, start_value, next_coarse[None, None])
    return fine_nodes, next_start, next_coarse


def solution(mesh):
    places = Places(mesh.shape["tm"], mesh.shape["space"])
    return jax.shard_map(
        lambda *args: on_device(places, *args),
        mesh=mesh,
        in_specs=(
            P("tm", "space", None, None),
            P("tm", None, "space", None, None),
            P("space", None, None),
        ),
        out_specs=(
            P("tm", None, "space", None, None),
            P("tm", "space", None, None),
            P("tm", "space", None, None),
        ),
        check_vma=False,
    )
```

```python
import math

import jax
import jax.numpy as jnp
from jax import lax
from jax.experimental import pallas as pl
from jax.experimental.pallas import tpu as pltpu
from jax.sharding import PartitionSpec as P

AXES = ("tm", "space")
STEP = 2.0
ROOT_SIX = math.sqrt(6.0)
NODE_TIMES = [(4.0 - ROOT_SIX) / 10.0, (4.0 + ROOT_SIX) / 10.0, 1.0]
COLLOC = [
    [
        (88.0 - 7.0 * ROOT_SIX) / 360.0,
        (296.0 - 169.0 * ROOT_SIX) / 1800.0,
        (-2.0 + 3.0 * ROOT_SIX) / 225.0,
    ],
    [
        (296.0 + 169.0 * ROOT_SIX) / 1800.0,
        (88.0 + 7.0 * ROOT_SIX) / 360.0,
        (-2.0 - 3.0 * ROOT_SIX) / 225.0,
    ],
    [(16.0 - ROOT_SIX) / 36.0, (16.0 + ROOT_SIX) / 36.0, 1.0 / 9.0],
]
ROWS = 16
KINDS = 16
LANES = 128
SCOPED = 8 * 2**20


def sweep_weight(row, column):
    below = COLLOC[row - 1][column] if row > 0 else 0.0
    return COLLOC[row][column] - below


def node_width(row):
    below = NODE_TIMES[row - 1] if row > 0 else 0.0
    return NODE_TIMES[row] - below


class Places:
    def __init__(self, slices, planes):
        self.slices, self.planes = slices, planes
        self.crossed = slices % 2 == 0 and planes % 2 == 0

    def flat(self, t, s):
        return t * self.planes + s

    def device(self, t, p):
        if not self.crossed:
            return self.flat(t, p)
        return self.flat(2 * (t // 2) + p % 2, 2 * (p // 2) + t % 2)

    def every(self):
        return [(t, p) for t in range(self.slices) for p in range(self.planes)]

    def swap(self):
        return [(self.flat(t, p), self.device(t, p)) for t, p in self.every()]

    def to_next(self):
        return [(self.device(t, p), self.flat(t + 1, p)) for t, p in self.every() if t + 1 < self.slices]

    def pairs(self, odd):
        partner = lambda p: p + 1 if p % 2 == odd else p - 1
        return [
            (self.device(t, p), self.device(t, partner(p)))
            for t, p in self.every()
            if 0 <= partner(p) < self.planes
        ]

    def rounds(self):
        left, stride, found = self.planes, 1, []
        while left > 1:
            factor = next(f for f in range(2, left + 1) if left % f == 0)
            turns = []
            for turn in range(1, factor):
                moved = lambda p: p + (((p // stride + turn) % factor) - (p // stride) % factor) * stride
                turns.append([(self.device(t, p), self.device(t, moved(p))) for t, p in self.every()])
            found.append(turns)
            left, stride = left // factor, stride * factor
        return found


def own_plane(places):
    t, s = lax.axis_index("tm"), lax.axis_index("space")
    return 2 * (s // 2) + t % 2 if places.crossed else s


def move(value, perm):
    return lax.ppermute(value, AXES, perm)


def row_after(ref, lead, start, count):
    total = ref.shape[-2]
    if start + count + 1 <= total:
        return ref[(*lead, slice(start + 1, start + count + 1), slice(None))]
    return pltpu.roll(ref[(*lead, slice(start, start + count), slice(None))], count - 1, 0)


def row_before(ref, lead, start, count):
    if start > 0:
        return ref[(*lead, slice(start - 1, start + count - 1), slice(None))]
    return pltpu.roll(ref[(*lead, slice(0, count), slice(None))], 1, 0)


def heat_rows(own, lead, beside, faces, start, count):
    rows = slice(start, start + count)
    here = own[(*lead, rows, slice(None))]
    width = here.shape[-1]
    face_x = faces[3, rows, :]
    result = faces[0, rows, :] * beside[0] + faces[1, rows, :] * beside[1]
    result += faces[2, rows, :] * row_after(own, lead, start, count)
    lower = row_before(faces, (2,), start, count) * row_before(own, lead, start, count)
    if start == 0:
        lower = jnp.where(lax.broadcasted_iota(jnp.int32, lower.shape, 0) == 0, 0.0, lower)
    result += lower
    result += face_x * pltpu.roll(here, width - 1, 1) + pltpu.roll(face_x * here, 1, 1)
    return result - faces[4, rows, :] * here, here


def chunks(ref):
    total = ref.shape[-2]
    return [(start, min(ROWS, total - start)) for start in range(0, total, ROWS)]


def faces_kernel(kappa, kappa_a, kappa_b, faces):
    length, width = kappa.shape
    for start, count in chunks(kappa):
        rows = slice(start, start + count)
        here = kappa[rows, :]
        face_a = 0.5 * (here + kappa_a[rows, :])
        face_b = 0.5 * (here + kappa_b[rows, :])
        after = row_after(kappa, (), start, count)
        before = row_before(kappa, (), start, count)
        row = lax.broadcasted_iota(jnp.int32, here.shape, 0) + start
        column = lax.broadcasted_iota(jnp.int32, here.shape, 1)
        after = jnp.where(row == length - 1, 0.0, after)
        before = jnp.where(row == 0, 0.0, before)
        right = jnp.where(column == width - 1, 0.0, pltpu.roll(here, width - 1, 1))
        left = jnp.where(column == 0, 0.0, pltpu.roll(here, 1, 1))
        face_y = 0.5 * (here + after)
        face_x = 0.5 * (here + right)
        faces[0, rows, :] = face_a
        faces[1, rows, :] = face_b
        faces[2, rows, :] = jnp.where(row == length - 1, 0.0, face_y)
        faces[3, rows, :] = jnp.where(column == width - 1, 0.0, face_x)
        faces[4, rows, :] = face_a + face_b + face_y + face_x + 0.5 * (here + before) + 0.5 * (here + left)


def increments_kernel(begin, *refs):
    nodes, beside_a, beside_b, faces, outs = refs[:3], refs[3:6], refs[6:9], refs[9], refs[10:]
    for start, count in chunks(begin):
        rows = slice(start, start + count)
        images, values = [], [begin[rows, :]]
        for column in range(3):
            image, here = heat_rows(
                nodes[column], (), (beside_a[column][rows, :], beside_b[column][rows, :]), faces, start, count
            )
            images.append(image)
            values.append(here)
        for row in range(3):
            change = values[row] - values[row + 1]
            for column in range(3):
                change += (STEP * sweep_weight(row, column)) * images[column]
            outs[row][rows, :] = change


def apply_kernel(width, count_in, *refs):
    own, beside_a, beside_b = refs[:count_in], refs[count_in : 2 * count_in], refs[2 * count_in : 3 * count_in]
    faces, out = refs[3 * count_in], refs[3 * count_in + 1 :]
    field = own[0]
    if count_in > 1:
        field = out[1]
        for start, count in chunks(field):
            rows = slice(start, start + count)
            field[rows, :] = sum(ref[rows, :] for ref in own)
    for start, count in chunks(field):
        rows = slice(start, start + count)
        beside = (sum(ref[rows, :] for ref in beside_a), sum(ref[rows, :] for ref in beside_b))
        image, here = heat_rows(field, (), beside, faces, start, count)
        out[0][rows, :] = here - width * image


def folded(value):
    return jnp.sum(value.reshape(value.shape[0] // 8, 8, value.shape[1]), axis=0)


def whole_sum(value):
    return jnp.sum(jnp.sum(value, axis=0, keepdims=True), axis=1, keepdims=True)


def moments_kernel(width, place, residual, image, image_a, image_b, faces, out):
    zero = jnp.zeros((8, residual.shape[1]), jnp.float32)
    rr, rq, qq = zero, zero, zero
    for start, count in chunks(residual):
        rows = slice(start, start + count)
        r, q = residual[rows, :], image[rows, :]
        rr, rq, qq = rr + folded(r * r), rq + folded(r * q), qq + folded(q * q)
    rr, rq, qq = whole_sum(rr), whole_sum(rq), whole_sum(qq)
    centre = jnp.where(qq > 0.0, rq / jnp.where(qq > 0.0, qq, 1.0), 0.0)
    sums = [zero] * 6
    for start, count in chunks(residual):
        rows = slice(start, start + count)
        heat, q = heat_rows(image, (), (image_a[rows, :], image_b[rows, :]), faces, start, count)
        aq = q - width * heat
        w = residual[rows, :] - centre * q
        aw = q - centre * aq
        terms = (w * w, w * q, w * aw, w * aq, q * aw, q * aq)
        sums = [total + folded(term) for total, term in zip(sums, terms)]
    values = [rr, rq, qq, centre] + [whole_sum(total) for total in sums]
    kind = lax.broadcasted_iota(jnp.int32, out.shape, 0)
    lane = lax.broadcasted_iota(jnp.int32, out.shape, 1)
    message = jnp.zeros(out.shape, jnp.float32)
    for index, value in enumerate(values):
        message = jnp.where(kind == index, value, message)
    out[...] = jnp.where(lane == place[0], message, 0.0)


def step_weights(gathered):
    row = lambda index: gathered[index : index + 1, :]
    total = lambda value: jnp.sum(value, axis=1, keepdims=True)
    rr, rq = total(row(0)), total(row(1))
    step = rr / rq
    away = step - row(3)
    rr_next = total(row(4) - 2.0 * away * row(5) + away * away * row(2))
    energy = total(row(6) - away * (row(7) + row(8)) + away * away * row(9))
    momentum = rr_next / rr
    step_next = rr_next / (energy - momentum * rr_next / step)
    return step + step_next * (1.0 + momentum), -step_next * step


def advance_kernel(width, keep, gathered, guess, *refs):
    grown, residual, image, faces = refs[0:3], refs[3:6], refs[6:9], refs[9]
    result, product, following = refs[10], refs[11], refs[12:]
    first, second = step_weights(gathered[...])
    for start, count in chunks(guess):
        rows = slice(start, start + count)
        change = first * residual[0][rows, :] + second * image[0][rows, :]
        result[rows, :] = guess[rows, :] + change
        following[0][rows, :] = grown[0][rows, :] + change
    for start, count in chunks(guess):
        rows = slice(start, start + count)
        beside = []
        for side in (1, 2):
            value = grown[side][rows, :] + first * residual[side][rows, :] + second * image[side][rows, :]
            if keep:
                following[side][rows, :] = value
            beside.append(value)
        heat, here = heat_rows(following[0], (), beside, faces, start, count)
        product[rows, :] = here - width * heat


def finish_kernel(gathered, guess, residual, image, out):
    first, second = step_weights(gathered[...])
    for start, count in chunks(guess):
        rows = slice(start, start + count)
        out[rows, :] = guess[rows, :] + first * residual[rows, :] + second * image[rows, :]


VMEM = pl.BlockSpec(memory_space=pltpu.VMEM)
SMEM = pl.BlockSpec(memory_space=pltpu.SMEM)


def call(kernel, shapes, *args, scalars=0):
    single = not isinstance(shapes, list)
    outs = [pltpu.VMEM(shape, jnp.float32) for shape in ([shapes] if single else shapes)]
    args = [
        arg if index < scalars else pltpu.with_memory_space_constraint(arg, pltpu.VMEM)
        for index, arg in enumerate(args)
    ]
    found = pl.pallas_call(
        kernel,
        out_shape=outs,
        in_specs=[SMEM] * scalars + [VMEM] * (len(args) - scalars),
        out_specs=[VMEM] * len(outs),
        compiler_params=pltpu.CompilerParams(vmem_limit_bytes=SCOPED),
    )(*args)
    return found[0] if single else found


def on_device(places, start_value, old_nodes, diffusivity):
    plane = diffusivity.shape[1:]
    swap, near, far = places.swap(), places.pairs(0), places.pairs(1)
    place = own_plane(places).astype(jnp.int32).reshape(1)

    def sides(value):
        return move(value, far), move(value, near)

    def gather(message):
        for turns in places.rounds():
            message = sum([move(message, perm) for perm in turns], message)
        return message

    def moments(width, residual, image, beside, faces):
        lanes = LANES * (-(-places.planes // LANES))
        return call(
            lambda *refs: moments_kernel(width, *refs),
            (KINDS, lanes),
            place,
            residual,
            image,
            *beside,
            faces,
            scalars=1,
        )

    kappa = move(diffusivity[0], swap)
    nodes = [move(old_nodes[0, column, 0], swap) for column in range(3)]
    begin = move(start_value[0, 0], swap)
    kappa_sides = sides(kappa)
    node_sides = [sides(node) for node in nodes]
    faces = call(faces_kernel, (5, *plane), kappa, *kappa_sides)
    grown = call(
        increments_kernel,
        [plane] * 3,
        begin,
        *nodes,
        *[pair[0] for pair in node_sides],
        *[pair[1] for pair in node_sides],
        faces,
    )
    grown_sides = [sides(value) for value in grown]
    trio = [(grown[m], *grown_sides[m]) for m in range(3)]
    widths = [STEP * node_width(row) for row in range(3)]

    residual = trio[0]
    image = call(lambda *refs: apply_kernel(widths[0], 1, *refs), plane, *residual, faces)
    image_trio = (image, *sides(image))
    fresh = []
    for row in range(2):
        gathered = gather(moments(widths[row], residual[0], image, image_trio[1:], faces))
        keep = row == 0
        found = call(
            lambda *refs: advance_kernel(widths[row + 1], keep, *refs),
            [plane] * (5 if keep else 3),
            gathered,
            nodes[row],
            *trio[row + 1],
            *residual,
            *image_trio,
            faces,
        )
        fresh.append(found[0])
        image, residual = found[1], found[2:]
        image_trio = (image, *sides(image))
    gathered = gather(moments(widths[2], residual[0], image, image_trio[1:], faces))
    fresh.append(call(finish_kernel, plane, gathered, nodes[2], residual[0], image))

    coarse_image, coarse = call(
        lambda *refs: apply_kernel(STEP, 3, *refs),
        [plane] * 2,
        *grown,
        *[pair[0] for pair in grown_sides],
        *[pair[1] for pair in grown_sides],
        faces,
    )
    coarse_gathered = gather(moments(STEP, coarse, coarse_image, sides(coarse_image), faces))
    coarse_end = call(finish_kernel, plane, coarse_gathered, nodes[2], coarse, coarse_image)

    next_coarse = move(coarse_end, places.to_next())
    next_start = move(fresh[2], places.to_next())
    fine_nodes = jnp.stack([move(value, swap) for value in fresh])[None, :, None]
    first_slice = lax.axis_index("tm") == 0
    next_start = jnp.where(first_slice, start_value, next_start[None, None])
    next_coarse = jnp.where(first_slice, start_value, next_coarse[None, None])
    return fine_nodes, next_start, next_coarse


def solution(mesh):
    places = Places(mesh.shape["tm"], mesh.shape["space"])
    return jax.shard_map(
        lambda *args: on_device(places, *args),
        mesh=mesh,
        in_specs=(
            P("tm", "space", None, None),
            P("tm", None, "space", None, None),
            P("space", None, None),
        ),
        out_specs=(
            P("tm", None, "space", None, None),
            P("tm", "space", None, None),
            P("tm", "space", None, None),
        ),
        check_vma=False,
    )
```
